32 devices in a mesh: lat: 4 (over y, x), lon: 8 (over z, core).
Axes of the slice: x: 2, y: 2, z: 4, core: 2. Of those that a mesh axis runs over, the one named last changes fastest.
Arguments:
- block_input: float32 [96, 192, 384], P('lat', 'lon'), may hold values from -90 to 90, as said below
- cotangent: float32 [96, 192, 384], P('lat', 'lon'), may hold values from -6 to 6
- weights: float32 [1769472], replicated, may hold values from -4 to 4, as said below
- first_moment: float32 [1769472], P(('lat', 'lon')), may hold values from -3 to 3
- second_moment: float32 [1769472], P(('lat', 'lon')), may hold values from 0.05 to 2
- bias_table: float32 [12, 529], replicated, may hold values from -5 to 5
- bias_index: int32 [144, 144], replicated, may hold values from 0 to 528
- region_ids: int32 [96, 192], P('lat', 'lon'), may hold values from 0 to 2
Outputs:
- grad_input: float32 [96, 192, 384], P('lat', 'lon')
- weights_new: float32 [1769472], replicated
- first_new: float32 [1769472], P(('lat', 'lon'))
- second_new: float32 [1769472], P(('lat', 'lon'))
- table_grad: float32 [12, 529], replicated
The draws below stay inside these ranges and needn't reach their ends.
Inputs may be any that keep to these rules, and one draw needn't show every extreme that they name: `block_input`: Tokens' features; real values. `weights`: real values. `region_ids`: entry (r, c) is the region of the token at ((r + 6) mod 96, (c + 6) mod 192) of the input grid.
All inputs are finite; a program needn't handle non-finite values.
Results may differ from the reference program's by a relative error of at most 0.0003.
Values sent between devices are 32-bit elements; how exact they have to be, the bound alone decides.
A program may use at most 128 MiB of HBM per device.

```python
import math
import jax
import jax.numpy as jnp
from jax import lax

D = 384
HEADS = 12
FF = 1536
WIN = 12
HEAD_DIM = 32
SHIFT = 6
BIAS = 529
NPARAM = 1769472
LAT = 96
LON = 192
TOKENS = 18432


def draw_block_input(key, part):
    streams = jax.random.split(jax.random.fold_in(key, 7), 1)
    sample = jax.random.normal(streams[0], (LAT, LON, D), jnp.float32)
    return jnp.clip(sample, -90.0, 90.0)


def draw_weights(key, part):
    streams = jax.random.split(jax.random.fold_in(key, 13), 6)
    query = jax.random.normal(streams[0], (D, D), jnp.float32) * D ** (-0.5)
    keyed = jax.random.normal(streams[1], (D, D), jnp.float32) * D ** (-0.5)
    valued = jax.random.normal(streams[2], (D, D), jnp.float32) * D ** (-0.5)
    w_proj = jax.random.normal(streams[3], (D, D), jnp.float32) * D ** (-0.5)
    w_up = jax.random.normal(streams[4], (D, FF), jnp.float32) * D ** (-0.5)
    w_down = jax.random.normal(streams[5], (FF, D), jnp.float32) * FF ** (-0.5)
    w_qkv = jnp.concatenate([query, keyed, valued], axis=1)
    packed = jnp.concatenate([w_qkv.reshape(-1), w_proj.reshape(-1), w_up.reshape(-1), w_down.reshape(-1)])
    return jnp.clip(packed, -4.0, 4.0)


def place_ends(drawn, own_key, smallest, largest):
    extent = drawn.shape
    index_at = [jax.random.randint(jax.random.fold_in(own_key, axis), (), 0, extent[axis]) for axis in range(len(extent))]
    drawn = drawn.at[tuple(index_at)].set(smallest)
    longest = extent.index(max(extent))
    index_at[longest] = (index_at[longest] + 1) % extent[longest]
    return drawn.at[tuple(index_at)].set(largest)


def levels(own_key, extent, shards, smallest, largest):
    gain = 1.0
    for axis_at, parts in shards:
        heights = jax.random.uniform(jax.random.fold_in(jax.random.fold_in(own_key, 6), axis_at), (parts,), jnp.float32, smallest / len(shards), largest / len(shards))
        gain = gain * jnp.repeat(jnp.exp(heights), extent[axis_at] // parts).reshape((-1,) + (1,) * (len(extent) - 1 - axis_at))
    return gain


def bell_draw(key, extent, scale, limit, cuts=(), dtype=jnp.bfloat16):
    gain = levels(key, extent, cuts, -0.22, 0.18) if cuts else 1.0
    values = jax.random.normal(key, extent, jnp.float32) * scale * gain
    return jnp.minimum(jnp.maximum(values, -limit), limit).astype(dtype)


def setup_inputs(seed: int = 0) -> dict:
    arg_keys = jax.random.split(jax.random.key(seed), 9)
    block_input = draw_block_input(jax.random.fold_in(arg_keys[8], 71), 0)
    cotangent = bell_draw(arg_keys[1], (LAT, LON, D), 1.0, 6.0, ((0, 4), (1, 8)), jnp.float32)
    weights = draw_weights(jax.random.fold_in(arg_keys[8], 71), 0)
    first_moment = bell_draw(arg_keys[3], (NPARAM,), 0.5, 3.0, ((0, 32),), jnp.float32)
    second_moment = jnp.clip(jnp.exp(math.log(2.0) - 3.6888794 * jax.random.uniform(arg_keys[4], (NPARAM,), jnp.float32) ** levels(arg_keys[4], (NPARAM,), ((0, 32),), -0.2, 0.2)), 0.05, 2.0)
    bias_table = bell_draw(arg_keys[5], (HEADS, BIAS), 1.0, 5.0, (), jnp.float32)
    bias_index = place_ends(jax.random.randint(arg_keys[6], (WIN * WIN, WIN * WIN), 0, BIAS), jax.random.fold_in(arg_keys[6], 1), 0, BIAS - 1).astype(jnp.int32)
    region_ids = place_ends(jax.random.randint(arg_keys[7], (LAT, LON), 0, 3), jax.random.fold_in(arg_keys[7], 1), 0, 2).astype(jnp.int32)
    return dict(block_input=block_input, cotangent=cotangent, weights=weights, first_moment=first_moment, second_moment=second_moment, bias_table=bias_table, bias_index=bias_index, region_ids=region_ids)


precise = lax.Precision.HIGHEST

def normalize(values):
    center = values - lax.optimization_barrier(jnp.mean(values, axis=-1, keepdims=True))
    spread = lax.optimization_barrier(jnp.mean(center * center, axis=-1, keepdims=True))
    return center / jnp.sqrt(spread + 1e-05)

def windows(tensor):
    height, breadth, features = tensor.shape
    blocks = tensor.reshape(height // WIN, WIN, breadth // WIN, WIN, features)
    return blocks.transpose(0, 2, 1, 3, 4).reshape(-1, WIN * WIN, features)

def unwindow(blocks, height, breadth):
    features = blocks.shape[-1]
    tensor = blocks.reshape(height // WIN, breadth // WIN, WIN, WIN, features)
    return tensor.transpose(0, 2, 1, 3, 4).reshape(height, breadth, features)

def unpack(packed):
    first_cut = D * 3 * D
    second_cut = first_cut + D * D
    third_cut = second_cut + D * FF
    return (packed[:first_cut].reshape(D, 3 * D), packed[first_cut:second_cut].reshape(D, D), packed[second_cut:third_cut].reshape(D, FF), packed[third_cut:].reshape(FF, D))

def attend(tensor, w_all, bias_table, bias_index, region_ids, wrapped):
    w_qkv, w_proj, _, _ = unpack(w_all)
    height, breadth, _ = tensor.shape
    flat_rows = normalize(tensor).reshape(-1, D)
    mixed = jnp.dot(flat_rows, w_qkv, precision=precise, preferred_element_type=jnp.float32)
    mixed = windows(mixed.reshape(height, breadth, 3 * D))
    window_count = mixed.shape[0]
    query = mixed[:, :, :D].reshape(window_count, WIN * WIN, HEADS, HEAD_DIM)
    keyed = mixed[:, :, D:2 * D].reshape(window_count, WIN * WIN, HEADS, HEAD_DIM)
    valued = mixed[:, :, 2 * D:].reshape(window_count, WIN * WIN, HEADS, HEAD_DIM)
    scores = jnp.einsum('wihd,wjhd->whij', query, keyed, precision=precise) / math.sqrt(HEAD_DIM)
    scores = scores + jnp.take(bias_table, bias_index, axis=1)[None]
    labels = windows(region_ids[:, :, None])[:, :, 0]
    halves = windows(jnp.broadcast_to(wrapped[:, None, None], (height, breadth, 1)).astype(jnp.int32))[:, :, 0]
    allowed = (labels[:, :, None] == labels[:, None, :]) & (halves[:, :, None] == halves[:, None, :])
    allowed = allowed[:, None]
    masked = jnp.where(allowed, scores, -jnp.inf)
    summit = lax.stop_gradient(lax.optimization_barrier(jnp.max(masked, axis=-1, keepdims=True)))
    raised = jnp.exp(masked - summit)
    probability = raised / lax.optimization_barrier(jnp.sum(raised, axis=-1, keepdims=True))
    context = jnp.einsum('whij,wjhd->wihd', probability, valued, precision=precise)
    context = unwindow(context.reshape(window_count, WIN * WIN, D), height, breadth).reshape(-1, D)
    return jnp.dot(context, w_proj, precision=precise, preferred_element_type=jnp.float32).reshape(height, breadth, D)

def feed(tensor, w_all):
    _, _, w_up, w_down = unpack(w_all)
    flat_rows = normalize(tensor).reshape(-1, D)
    hidden = jax.nn.gelu(jnp.dot(flat_rows, w_up, precision=precise, preferred_element_type=jnp.float32), approximate=True)
    return jnp.dot(hidden, w_down, precision=precise, preferred_element_type=jnp.float32).reshape(tensor.shape)

def reference(block_input, cotangent, weights, first_moment, second_moment, bias_table, bias_index, region_ids):
    wrapped = jnp.arange(LAT) >= LAT - SHIFT

    def forward(tensor, w_all, table):
        moved = jnp.roll(tensor, (-SHIFT, -SHIFT), (0, 1))
        mixed = moved + attend(moved, w_all, table, bias_index, region_ids, wrapped)
        output = mixed + feed(mixed, w_all)
        return jnp.roll(output, (SHIFT, SHIFT), (0, 1))
    _, pullback = jax.vjp(forward, block_input, weights, bias_table)
    grad_input, grad_weights, grad_table = pullback(cotangent)
    factor = 1.0 / math.sqrt(TOKENS)
    grad_weights = grad_weights * factor
    first_new = 0.9 * first_moment + 0.1 * grad_weights
    second_new = 0.95 * second_moment + 0.05 * grad_weights * grad_weights
    weights_new = weights - 0.01 * first_new / (jnp.sqrt(second_new) + 1e-08)
    return (grad_input, weights_new, first_new, second_new, grad_table * factor)
```

```python
import functools
import math

import jax
import jax.numpy as jnp
from jax import lax
from jax.experimental import pallas as pl
from jax.experimental.pallas import tpu as pltpu
from jax.sharding import PartitionSpec as P

D = 384
HEADS = 12
FF = 1536
WIN = 12
HEAD_DIM = 32
SHIFT = 6
TOK = WIN * WIN
LOW = 32
HEAD_ROWS = 16

high = lax.Precision.HIGH
F32 = jnp.float32
BF16 = jnp.bfloat16
NN = (((1,), (0,)), ((), ()))
NT = (((1,), (1,)), ((), ()))
TN = (((0,), (0,)), ((), ()))


def passed_along(value, axis, by):
    size = lax.axis_size(axis)
    return lax.ppermute(value, axis, [(i, (i + by) % size) for i in range(size)])


def windows(tensor):
    height, breadth, features = tensor.shape
    blocks = tensor.reshape(height // WIN, WIN, breadth // WIN, WIN, features)
    return blocks.transpose(0, 2, 1, 3, 4).reshape(-1, WIN * WIN, features)


def unwindow(blocks, height, breadth):
    features = blocks.shape[-1]
    tensor = blocks.reshape(height // WIN, breadth // WIN, WIN, WIN, features)
    return tensor.transpose(0, 2, 1, 3, 4).reshape(height, breadth, features)


def unpack(packed):
    first_cut = D * 3 * D
    second_cut = first_cut + D * D
    third_cut = second_cut + D * FF
    return (
        packed[:first_cut].reshape(D, 3 * D),
        packed[first_cut:second_cut].reshape(D, D),
        packed[second_cut:third_cut].reshape(D, FF),
        packed[third_cut:].reshape(FF, D),
    )


def split(value):
    upper = value.astype(BF16)
    return upper, (value - upper.astype(F32)).astype(BF16)


def mul(a, b, dims):
    return lax.dot_general(a, b, dims, preferred_element_type=F32)


def dot3(a, b, dims):
    return mul(a[0], b[0], dims) + mul(a[0], b[1], dims) + mul(a[1], b[0], dims)


def head_of(pair, h):
    at = h * HEAD_DIM
    return pair[0][:, at : at + HEAD_DIM], pair[1][:, at : at + HEAD_DIM]


def attention_forward_kernel(qkv_ref, bias_ref, row_ref, col_ref, context_ref, prob_ref):
    q = split(qkv_ref[0, :, :D] * (1.0 / math.sqrt(HEAD_DIM)))
    k = split(qkv_ref[0, :, D : 2 * D])
    v = split(qkv_ref[0, :, 2 * D :])
    allowed = col_ref[0] == row_ref[0]
    parts = []
    for h in range(HEADS):
        scores = dot3(head_of(q, h), head_of(k, h), NT) + bias_ref[h]
        masked = jnp.where(allowed, scores, -jnp.inf)
        raised = jnp.exp(masked - jnp.max(masked, axis=-1, keepdims=True))
        prob = raised / jnp.sum(raised, axis=-1, keepdims=True)
        prob_ref[0, h] = prob
        parts.append(dot3(split(prob), head_of(v, h), NN))
    context_ref[0] = jnp.concatenate(parts, axis=1)


def attention_backward_kernel(qkv_ref, prob_ref, grad_ref, dqkv_ref, dbias_ref):
    @pl.when(pl.program_id(0) == 0)
    def _():
        dbias_ref[...] = jnp.zeros_like(dbias_ref)

    scale = 1.0 / math.sqrt(HEAD_DIM)
    q = split(qkv_ref[0, :, :D])
    k = split(qkv_ref[0, :, D : 2 * D])
    v = split(qkv_ref[0, :, 2 * D :])
    g = split(grad_ref[0])
    dq, dk, dv = [], [], []
    for h in range(HEADS):
        prob = prob_ref[0, h]
        g_h = head_of(g, h)
        dv.append(dot3(split(prob), g_h, TN))
        dprob = dot3(g_h, head_of(v, h), NT)
        dscore = prob * (dprob - jnp.sum(prob * dprob, axis=-1, keepdims=True))
        dbias_ref[h] += dscore
        dscore = split(dscore * scale)
        dq.append(dot3(dscore, head_of(k, h), NN))
        dk.append(dot3(dscore, head_of(q, h), TN))
    dqkv_ref[0] = jnp.concatenate(dq + dk + dv, axis=1)


def bias_kernel(levels, table_ref, index_ref, bias_ref):
    upper, lower = split(table_ref[...])
    rows = lax.broadcasted_iota(jnp.int32, (LOW, TOK), 0)
    for r in range(index_ref.shape[0]):
        index = index_ref[r : r + 1, :]
        low = index & (LOW - 1)
        high_part = index >> 5
        hot = jnp.where(rows == low, 1.0, 0.0).astype(BF16)
        spread = mul(upper, hot, NN) + mul(lower, hot, NN)
        total = jnp.zeros((HEAD_ROWS, TOK), F32)
        for level in range(levels):
            total = jnp.where(
                high_part == level, spread[level * HEAD_ROWS : (level + 1) * HEAD_ROWS], total
            )
        bias_ref[:, r, :] = total[:HEADS]


def table_kernel(levels, grad_ref, index_ref, table_ref):
    @pl.when(pl.program_id(0) == 0)
    def _():
        table_ref[...] = jnp.zeros_like(table_ref)

    rows = lax.broadcasted_iota(jnp.int32, (LOW, TOK), 0)
    for r in range(index_ref.shape[0]):
        index = index_ref[r : r + 1, :]
        low = index & (LOW - 1)
        high_part = index >> 5
        hot = jnp.where(rows == low, 1.0, 0.0).astype(BF16)
        grad = jnp.concatenate(
            [grad_ref[:, r, :], jnp.zeros((HEAD_ROWS - HEADS, TOK), F32)], axis=0
        )
        stacked = jnp.concatenate(
            [jnp.where(high_part == level, grad, 0.0) for level in range(levels)], axis=0
        )
        upper, lower = split(stacked)
        table_ref[...] += mul(upper, hot, NT) + mul(lower, hot, NT)


def attention_forward(qkv, bias, row_label, col_label):
    count = qkv.shape[0]
    return pl.pallas_call(
        attention_forward_kernel,
        grid=(count,),
        in_specs=[
            pl.BlockSpec((1, TOK, 3 * D), lambda w: (w, 0, 0)),
            pl.BlockSpec((HEADS, TOK, TOK), lambda w: (0, 0, 0)),
            pl.BlockSpec((1, 1, TOK), lambda w: (w, 0, 0)),
            pl.BlockSpec((1, TOK, 1), lambda w: (w, 0, 0)),
        ],
        out_specs=(
            pl.BlockSpec((1, TOK, D), lambda w: (w, 0, 0)),
            pl.BlockSpec((1, HEADS, TOK, TOK), lambda w: (w, 0, 0, 0)),
        ),
        out_shape=(
            jax.ShapeDtypeStruct((count, TOK, D), F32),
            jax.ShapeDtypeStruct((count, HEADS, TOK, TOK), F32),
        ),
        cost_estimate=pl.CostEstimate(
            flops=40000000 * count, bytes_accessed=4000000 * count, transcendentals=250000 * count
        ),
    )(qkv, bias, row_label, col_label)


def attention_backward(qkv, prob, grad):
    count = qkv.shape[0]
    return pl.pallas_call(
        attention_backward_kernel,
        grid=(count,),
        in_specs=[
            pl.BlockSpec((1, TOK, 3 * D), lambda w: (w, 0, 0)),
            pl.BlockSpec((1, HEADS, TOK, TOK), lambda w: (w, 0, 0, 0)),
            pl.BlockSpec((1, TOK, D), lambda w: (w, 0, 0)),
        ],
        out_specs=(
            pl.BlockSpec((1, TOK, 3 * D), lambda w: (w, 0, 0)),
            pl.BlockSpec((HEADS, TOK, TOK), lambda w: (0, 0, 0)),
        ),
        out_shape=(
            jax.ShapeDtypeStruct((count, TOK, 3 * D), F32),
            jax.ShapeDtypeStruct((HEADS, TOK, TOK), F32),
        ),
        cost_estimate=pl.CostEstimate(
            flops=80000000 * count, bytes_accessed=4000000 * count, transcendentals=0
        ),
    )(qkv, prob, grad)


def look_up(table, index):
    entries = table.shape[1]
    levels = -(-entries // LOW)
    padded = jnp.pad(table, ((0, HEAD_ROWS - HEADS), (0, levels * LOW - entries)))
    padded = padded.reshape(HEAD_ROWS, levels, LOW).transpose(1, 0, 2).reshape(-1, LOW)
    return pl.pallas_call(
        functools.partial(bias_kernel, levels),
        grid=(TOK // 8,),
        in_specs=[
            pl.BlockSpec((levels * HEAD_ROWS, LOW), lambda i: (0, 0)),
            pl.BlockSpec((8, TOK), lambda i: (i, 0)),
        ],
        out_specs=pl.BlockSpec((HEADS, 8, TOK), lambda i: (0, i, 0)),
        out_shape=jax.ShapeDtypeStruct((HEADS, TOK, TOK), F32),
        cost_estimate=pl.CostEstimate(flops=1000000000, bytes_accessed=2000000, transcendentals=0),
    )(padded, index)


def table_gradient(grad, index, entries):
    levels = -(-entries // LOW)
    stacked = pl.pallas_call(
        functools.partial(table_kernel, levels),
        grid=(TOK // 8,),
        in_specs=[
            pl.BlockSpec((HEADS, 8, TOK), lambda i: (0, i, 0)),
            pl.BlockSpec((8, TOK), lambda i: (i, 0)),
        ],
        out_specs=pl.BlockSpec((levels * HEAD_ROWS, LOW), lambda i: (0, 0)),
        out_shape=jax.ShapeDtypeStruct((levels * HEAD_ROWS, LOW), F32),
        cost_estimate=pl.CostEstimate(flops=1000000000, bytes_accessed=2000000, transcendentals=0),
    )(grad, index)
    return stacked


def unstack_table(stacked, entries):
    levels = -(-entries // LOW)
    table = stacked.reshape(levels, HEAD_ROWS, LOW).transpose(1, 0, 2)
    return table.reshape(HEAD_ROWS, levels * LOW)[:HEADS, :entries]


def shift_ahead(stacked):
    from_east = passed_along(stacked[:, :, :SHIFT], "lon", -1)
    widened = jnp.concatenate([stacked[:, :, SHIFT:], from_east], axis=2)
    from_south = passed_along(widened[:, :SHIFT], "lat", -1)
    return jnp.concatenate([widened[:, SHIFT:], from_south], axis=1)


def shift_back(stacked):
    from_north = passed_along(stacked[:, -SHIFT:], "lat", 1)
    lengthened = jnp.concatenate([from_north, stacked[:, :-SHIFT]], axis=1)
    from_west = passed_along(lengthened[:, :, -SHIFT:], "lon", 1)
    return jnp.concatenate([from_west, lengthened[:, :, :-SHIFT]], axis=2)


def dense(a, b, dims):
    return lax.dot_general(a, b, dims, precision=high, preferred_element_type=F32)


def normalize(values):
    center = values - jnp.mean(values, axis=-1, keepdims=True)
    spread = jnp.mean(center * center, axis=-1, keepdims=True)
    inverse = 1.0 / jnp.sqrt(spread + 1e-05)
    return center * inverse, inverse


def normalize_backward(grad, normed, inverse):
    return inverse * (
        grad
        - jnp.mean(grad, axis=-1, keepdims=True)
        - normed * jnp.mean(grad * normed, axis=-1, keepdims=True)
    )


def per_device(
    block_input, cotangent, weights, first_moment, second_moment, bias_table, bias_index, region_ids
):
    tile_rows, tile_cols, _ = block_input.shape
    lat_count = lax.axis_size("lat")
    lon_count = lax.axis_size("lon")
    tokens = tile_rows * tile_cols
    entries = bias_table.shape[1]
    global_rows = lax.axis_index("lat") * tile_rows + jnp.arange(tile_rows)
    wrapped = global_rows >= tile_rows * lat_count - SHIFT
    labels = region_ids * 2 + wrapped[:, None].astype(jnp.int32)
    labels = windows(labels[:, :, None])[:, :, 0]

    bias = look_up(bias_table, bias_index)
    w_qkv, w_proj, w_up, w_down = unpack(weights)

    moved = shift_ahead(jnp.stack([block_input, cotangent]))
    x = windows(moved[0]).reshape(tokens, D)
    ct = windows(moved[1]).reshape(tokens, D)

    x_normed, x_inverse = normalize(x)
    qkv = dense(x_normed, w_qkv, NN).reshape(-1, TOK, 3 * D)
    context, prob = attention_forward(qkv, bias, labels[:, None, :], labels[:, :, None])
    context = context.reshape(tokens, D)
    mixed = x + dense(context, w_proj, NN)
    m_normed, m_inverse = normalize(mixed)
    hidden, gelu_back = jax.vjp(
        functools.partial(jax.nn.gelu, approximate=True), dense(m_normed, w_up, NN)
    )
    grad_down = dense(hidden, ct, TN)
    (d_up,) = gelu_back(dense(ct, w_down, NT))
    grad_up = dense(m_normed, d_up, TN)
    d_mixed = ct + normalize_backward(dense(d_up, w_up, NT), m_normed, m_inverse)
    grad_proj = dense(context, d_mixed, TN)
    d_context = dense(d_mixed, w_proj, NT).reshape(-1, TOK, D)
    d_qkv, d_bias = attention_backward(qkv, prob, d_context)
    d_qkv = d_qkv.reshape(tokens, 3 * D)
    grad_qkv = dense(x_normed, d_qkv, TN)
    grad_weights = jnp.concatenate(
        [g.reshape(-1) for g in (grad_qkv, grad_proj, grad_up, grad_down)]
    )

    factor = 1.0 / math.sqrt(tokens * lat_count * lon_count)
    shard_len = first_moment.shape[0]
    summed = lax.psum_scatter(grad_weights, "lat", scatter_dimension=0, tiled=True)
    summed = lax.psum_scatter(summed, "lon", scatter_dimension=0, tiled=True) * factor

    dx = d_mixed + normalize_backward(dense(d_qkv, w_qkv, NT), x_normed, x_inverse)
    dx = unwindow(dx.reshape(-1, TOK, D), tile_rows, tile_cols)
    grad_input = shift_back(dx[None])[0]
    table = table_gradient(d_bias, bias_index, entries)
    table_grad = unstack_table(lax.psum(table, ("lat", "lon")), entries) * factor

    owner_rank = lax.axis_index("lat") * lon_count + lax.axis_index("lon")
    own_weights = lax.dynamic_slice_in_dim(weights, owner_rank * shard_len, shard_len)
    first_new = 0.9 * first_moment + 0.1 * summed
    second_new = 0.95 * second_moment + 0.05 * summed * summed
    own_new = own_weights - 0.01 * first_new / (jnp.sqrt(second_new) + 1e-08)
    gathered = lax.all_gather(own_new, ("lat", "lon"), axis=0, tiled=True)
    return (grad_input, gathered, first_new, second_new, table_grad)


def solution(mesh):
    placed = (
        P("lat", "lon", None),
        P("lat", "lon", None),
        P(),
        P(("lat", "lon")),
        P(("lat", "lon")),
        P(),
        P(),
        P("lat", "lon"),
    )
    return jax.shard_map(
        per_device,
        mesh=mesh,
        in_specs=placed,
        out_specs=(P("lat", "lon", None), P(), P(("lat", "lon")), P(("lat", "lon")), P()),
        check_vma=False,
    )
```
